256 devices in a mesh: seq: 32 (over z, y), blk: 8 (over x, core).
Axes of the slice: x: 4, y: 4, z: 8, core: 2. Of those that a mesh axis runs over, the one named last changes fastest.
Arguments:
- q_latent: bfloat16 [64, 128, 512], P('blk', 'seq'), may hold values from -16 to 16
- q_rope: bfloat16 [64, 64, 128], P('blk', None, 'seq'), may hold values from -9 to 9
- cache_latent: bfloat16 [131072, 512], P(('seq', 'blk')), may hold values from -8 to 8
- cache_rope: bfloat16 [64, 131072], P(None, ('seq', 'blk')), may hold values from -6 to 6
- draft_latent: bfloat16 [64, 512], replicated, may hold values from -8 to 8
- draft_rope: bfloat16 [64, 64], replicated, may hold values from -6 to 6
- ancestors: int32 [64, 64], replicated, may hold values from 0 to 1, as said below
- valid_length: int32 [], replicated, may hold values from 65536 to 131072
- accepted: int32 [64], P('blk'), may hold values from 0 to 1, as said below
- w_value: bfloat16 [128, 512, 128], P('seq'), may hold values from -3 to 3
Outputs:
- attended: bfloat16 [64, 128, 128], P('blk', 'seq')
- accepted_total: int32 [], replicated
The draws below stay inside these ranges and needn't reach their ends.
Inputs may be any that keep to these rules, and one draw needn't show every extreme that they name: Node 0 is the root; every other node's parent has a lower index; ancestors[i, j] = 1 exactly when j is i or an ancestor of i. accepted is the row of ancestors of one node of the tree: that node and all of its ancestors.
All inputs are finite; a program needn't handle non-finite values.
Results may differ from the reference program's by a relative error of at most 0.02.
Values may be sent and summed in bfloat16 or wider, within the bound.
No kernel may reach another device: no remote copies, remote signals or barrier semaphores. Data moves between devices by JAX's collectives and lax.ppermute only.
A program may use at most 64 MiB of HBM per device.

```python
import jax
import jax.numpy as jnp
from jax import lax

HEADS = 128
LATENT = 512
ROPE = 64
VDIM = 128
DRAFT = 64
CACHE = 131072
N_BLK = 8


def shared_latents(key):
    base_key = jax.random.fold_in(key, 7)
    k_cache, k_query = jax.random.split(base_key, 2)
    cache = jnp.clip(jax.random.normal(k_cache, (CACHE, LATENT), jnp.float32), -6.0, 6.0)
    query = jnp.clip(1.5 * jax.random.normal(k_query, (DRAFT, HEADS, LATENT), jnp.float32), -9.0, 9.0)
    return (cache, query)


def draw_cache_latent(key, part):
    return shared_latents(key)[0].astype(jnp.bfloat16)


def draw_q_latent(key, part):
    return shared_latents(key)[1].astype(jnp.bfloat16)


def tree_tables(key):
    base_key = jax.random.fold_in(key, 13)
    k_parent, k_pick = jax.random.split(base_key)
    step = max(DRAFT // N_BLK, 1)
    nodes = jnp.arange(DRAFT, dtype=jnp.int32)
    lowest = jnp.maximum(nodes - step, 0)
    parent = jax.random.randint(k_parent, (DRAFT,), lowest, jnp.maximum(nodes, 1))
    identity = jnp.eye(DRAFT, dtype=jnp.int32)

    def extend(index, table):
        row = jnp.maximum(table[parent[index]], identity[index])
        return table.at[index].set(jnp.where(index > 0, row, identity[index]))
    table = lax.fori_loop(0, DRAFT, extend, identity)
    chosen = jax.random.randint(k_pick, (), DRAFT - step, DRAFT)
    return (table, table[chosen])


def draw_ancestors(key, part):
    return tree_tables(key)[0].astype(jnp.int32)


def draw_accepted(key, part):
    return tree_tables(key)[1].astype(jnp.int32)


def level_of(own_key, extent, cuts, smallest, top_value):
    factor_of, own = 1.0, jax.random.fold_in(own_key, 6)
    for dim, blocks in cuts:
        draws = jnp.exp(jax.random.uniform(jax.random.fold_in(own, dim), (blocks,), jnp.float32, smallest / len(cuts), top_value / len(cuts)))
        factor_of = factor_of * jnp.repeat(draws, extent[dim] // blocks).reshape([-1 if axis == dim else 1 for axis in range(len(extent))])
    return factor_of


def normal_values(rng, extent, scale, bound, cuts=(), kind=jnp.bfloat16):
    entries = scale * jax.random.normal(rng, extent, jnp.float32)
    if cuts:
        entries = entries * level_of(rng, extent, cuts, -0.22, 0.18)
    return jnp.clip(entries, -bound, bound).astype(kind)


def setup_inputs(seed: int = 0) -> dict:
    key_list = jax.random.split(jax.random.key(seed), 11)
    q_latent = draw_q_latent(jax.random.fold_in(key_list[10], 71), 0)
    q_rope = normal_values(key_list[1], (DRAFT, ROPE, HEADS), 1.5, 9.0, ((0, 8), (2, 32)))
    cache_latent = draw_cache_latent(jax.random.fold_in(key_list[10], 71), 0)
    cache_rope = normal_values(key_list[3], (ROPE, CACHE), 1.0, 6.0, ((1, 256),))
    draft_latent = normal_values(key_list[4], (DRAFT, LATENT), 1.3, 8.0)
    draft_rope = normal_values(key_list[5], (ROPE, DRAFT), 1.0, 6.0)
    ancestors = draw_ancestors(jax.random.fold_in(key_list[10], 71), 0)
    valid_length = jax.random.randint(key_list[7], (), CACHE // 2, CACHE + 1).astype(jnp.int32)
    accepted = draw_accepted(jax.random.fold_in(key_list[10], 71), 0)
    w_value = normal_values(key_list[9], (HEADS, LATENT, VDIM), 0.5, 3.0, ((0, 32),))
    return dict(q_latent=q_latent, q_rope=q_rope, cache_latent=cache_latent, cache_rope=cache_rope, draft_latent=draft_latent, draft_rope=draft_rope, ancestors=ancestors, valid_length=valid_length, accepted=accepted, w_value=w_value)


def reference(q_latent, q_rope, cache_latent, cache_rope, draft_latent, draft_rope, ancestors, valid_length, accepted, w_value):
    scale = (VDIM + ROPE) ** -0.5
    keys = cache_latent.astype(jnp.float32)
    rotary = cache_rope.astype(jnp.float32)
    draft_keys = draft_latent.astype(jnp.float32)
    draft_rot = draft_rope.astype(jnp.float32)
    live = jnp.arange(CACHE, dtype=jnp.int32) < valid_length
    tree = ancestors == 1
    width = min(8, HEADS)
    blocks = HEADS // width
    high = lax.Precision.HIGHEST

    def one_block(index):
        first = (index * width).astype(jnp.int32)
        query = lax.dynamic_slice_in_dim(q_latent, first, width, 1).astype(jnp.float32)
        qrot = lax.dynamic_slice_in_dim(q_rope, first, width, 2).astype(jnp.float32)
        weight = lax.dynamic_slice_in_dim(w_value, first, width, 0).astype(jnp.float32)
        cache_score = jnp.einsum("thl,sl->ths", query, keys, precision=high)
        cache_score = (cache_score + jnp.einsum("trh,rs->ths", qrot, rotary, precision=high)) * scale
        cache_score = jnp.where(live[None, None, :], cache_score, -1e30)
        draft_score = jnp.einsum("thl,jl->thj", query, draft_keys, precision=high)
        draft_score = (draft_score + jnp.einsum("trh,rj->thj", qrot, draft_rot, precision=high)) * scale
        draft_score = jnp.where(tree[:, None, :], draft_score, -1e30)
        peak = jnp.maximum(jnp.max(cache_score, axis=2), jnp.max(draft_score, axis=2))
        cache_w = jnp.exp(cache_score - peak[:, :, None])
        draft_w = jnp.exp(draft_score - peak[:, :, None])
        total = jnp.sum(cache_w, axis=2) + jnp.sum(draft_w, axis=2)
        latent_out = jnp.einsum("ths,sl->thl", cache_w, keys, precision=high)
        latent_out = latent_out + jnp.einsum("thj,jl->thl", draft_w, draft_keys, precision=high)
        latent_out = latent_out / total[:, :, None]
        return jnp.einsum("thl,hlv->thv", latent_out, weight, precision=high)

    stacked = lax.map(one_block, jnp.arange(blocks, dtype=jnp.int32))
    attended = jnp.transpose(stacked, (1, 0, 2, 3)).reshape(DRAFT, HEADS, VDIM)
    accepted_total = jnp.sum(accepted).astype(jnp.int32)
    return attended.astype(jnp.bfloat16), accepted_total
```

```python
import functools
import math

import jax
import jax.numpy as jnp
from jax import lax
from jax.experimental import pallas as pl
from jax.experimental.pallas import tpu as pltpu
from jax.sharding import Mesh
from jax.sharding import PartitionSpec as P

ROPE = 64
VDIM = 128
LATENT = 512
LANES = 128
SEQ = ("z", "y")
BLK = ("x", "core")
NEG = -1e30
SCALE2 = (VDIM + ROPE) ** -0.5 * math.log2(math.e)

ROWS = 32
Q_ROWS = 144
O_ROWS = 136
OWNERS = 8
BLOCK = OWNERS * ROWS


def dot(a, b, contract=((1,), (0,))):
    return lax.dot_general(a, b, (contract, ((), ())), preferred_element_type=jnp.float32)


def three_parts(value):
    high = value.astype(jnp.bfloat16)
    rest = value - high.astype(jnp.float32)
    middle = rest.astype(jnp.bfloat16)
    low = (rest - middle.astype(jnp.float32)).astype(jnp.bfloat16)
    return high, middle, low


def attend_kernel(n_chunks, limits_ref, q_ref, *refs):
    chunks, out_ref = refs[:n_chunks], refs[n_chunks]
    query, query_rope, key_rope, scores = refs[n_chunks + 1 :]
    rows = chunks[0].shape[0] - ROPE
    lane = lax.broadcasted_iota(jnp.int32, (ROPE, rows), 1)
    first_row = lax.broadcasted_iota(jnp.int32, (ROPE, rows), 0) == 0
    for c in range(n_chunks):
        here = slice(c * rows, (c + 1) * rows)
        key_rope[:ROPE, here] = chunks[c][rows:, :]
        dead = jnp.where(first_row & (lane >= limits_ref[c]), NEG, 0.0)
        key_rope[ROPE:, here] = dead.astype(jnp.bfloat16)
    one = lax.broadcasted_iota(jnp.int32, (BLOCK, ROPE), 1) == 0
    query_rope[:, ROPE:] = jnp.where(one, 1.0, 0.0).astype(jnp.bfloat16)
    own_lane = lax.broadcasted_iota(jnp.int32, (ROWS, LANES), 1)
    own_row = lax.broadcasted_iota(jnp.int32, (ROWS, LANES), 0)

    @pl.loop(0, q_ref.shape[0] // OWNERS)
    def _(step):
        for i in range(OWNERS):
            owner = step * OWNERS + i
            for j in range(4):
                query[i * ROWS : (i + 1) * ROWS, j * LANES : (j + 1) * LANES] = q_ref[
                    owner, j * ROWS : (j + 1) * ROWS, :
                ]
            both = q_ref[owner, 4 * ROWS :, :]
            query_rope[i * ROWS : i * ROWS + 16, :ROPE] = both[:, :ROPE]
            query_rope[i * ROWS + 16 : (i + 1) * ROWS, :ROPE] = both[:, ROPE:]
        peak = None
        for c in range(n_chunks):
            here = slice(c * rows, (c + 1) * rows)
            s = dot(query[...], chunks[c][:rows, :], ((1,), (1,)))
            s = s + dot(query_rope[...], key_rope[:, here])
            scores[:, here] = s
            for j in range(rows // LANES):
                part = s[:, j * LANES : (j + 1) * LANES]
                peak = part if peak is None else jnp.maximum(peak, part)
        peak = jnp.max(peak, axis=1, keepdims=True)
        total = jnp.zeros((BLOCK, LANES), jnp.float32)
        latent = jnp.zeros((BLOCK, LATENT), jnp.float32)
        for c in range(n_chunks):
            here = slice(c * rows, (c + 1) * rows)
            p = jnp.exp2((scores[:, here] - peak) * SCALE2)
            for j in range(rows // LANES):
                total = total + p[:, j * LANES : (j + 1) * LANES]
            latent = latent + dot(p.astype(jnp.bfloat16), chunks[c][:rows, :])
        total = jnp.sum(total, axis=1, keepdims=True)
        latent = (latent * (1.0 / total)).astype(jnp.bfloat16)
        lse = peak * SCALE2 + jnp.log2(total)
        for i in range(OWNERS):
            owner = step * OWNERS + i
            mine = slice(i * ROWS, (i + 1) * ROWS)
            for j in range(4):
                out_ref[owner, j * ROWS : (j + 1) * ROWS, :] = latent[
                    mine, j * LANES : (j + 1) * LANES
                ]
            line = jnp.where(own_lane == own_row, lse[mine, :], 0.0)
            line = jnp.sum(line, axis=0, keepdims=True)
            parts = jnp.concatenate([p.astype(jnp.float32) for p in three_parts(line)], axis=0)
            parts = jnp.concatenate([parts, jnp.zeros((5, LANES), jnp.float32)], axis=0)
            out_ref[owner, 4 * ROWS :, :] = parts.astype(jnp.bfloat16)


def attend(limits, queries, chunks):
    n = len(chunks)
    rows = chunks[0].shape[0] - ROPE
    vmem = pl.BlockSpec(memory_space=pltpu.VMEM)
    owners = queries.shape[0]
    return pl.pallas_call(
        functools.partial(attend_kernel, n),
        out_shape=jax.ShapeDtypeStruct((owners, O_ROWS, LANES), jnp.bfloat16),
        in_specs=[pl.BlockSpec(memory_space=pltpu.SMEM)] + [vmem] * (1 + n),
        out_specs=vmem,
        scratch_shapes=[
            pltpu.VMEM((BLOCK, LATENT), jnp.bfloat16),
            pltpu.VMEM((BLOCK, LANES), jnp.bfloat16),
            pltpu.VMEM((2 * ROPE, n * rows), jnp.bfloat16),
            pltpu.VMEM((BLOCK, n * rows), jnp.float32),
        ],
        compiler_params=pltpu.CompilerParams(vmem_limit_bytes=40 * 2**20),
        cost_estimate=pl.CostEstimate(
            flops=owners * ROWS * n * rows * 2 * 1280, bytes_accessed=8 * 2**20, transcendentals=0
        ),
        name="attend",
    )(limits, queries, *chunks)


def finish_kernel(tokens, heads, pieces_ref, q_ref, d_lat_ref, d_rope_ref, tree_ref, w_ref, out_ref):
    n = pieces_ref.shape[0]
    parts = pieces_ref[:, 4 * ROWS :, :].astype(jnp.float32)
    lse = parts[:, 0, :] + parts[:, 1, :] + parts[:, 2, :]
    query = jnp.concatenate([q_ref[j * ROWS : (j + 1) * ROWS, :] for j in range(4)], axis=1)
    both = q_ref[4 * ROWS :, :]
    query_rope = jnp.concatenate([both[:, :ROPE], both[:, ROPE:]], axis=0)
    draft = d_lat_ref[...]
    score = dot(query, draft, ((1,), (1,))) + dot(query_rope, d_rope_ref[...])
    tree = jnp.concatenate([tree_ref[...]] * heads, axis=0)
    score = jnp.where(tree == 1, score * SCALE2, NEG)
    draft_peak = jnp.max(score, axis=1, keepdims=True)
    own_lane = lax.broadcasted_iota(jnp.int32, (ROWS, LANES), 1)
    own_row = lax.broadcasted_iota(jnp.int32, (ROWS, LANES), 0)
    diagonal = own_lane == own_row

    def to_rows(line):
        return jnp.sum(jnp.where(diagonal, line, 0.0), axis=1, keepdims=True)

    cache_peak = to_rows(jnp.max(lse, axis=0, keepdims=True))
    peak = jnp.maximum(cache_peak, draft_peak)
    weight = jnp.exp2(score - peak)
    total = jnp.sum(weight, axis=1, keepdims=True)
    latent = dot(weight.astype(jnp.bfloat16), draft)
    for i in range(n):
        share = jnp.exp2(to_rows(lse[i : i + 1, :]) - peak)
        total = total + share
        piece = jnp.concatenate(
            [pieces_ref[i, j * ROWS : (j + 1) * ROWS, :] for j in range(4)], axis=1
        )
        latent = latent + share * piece.astype(jnp.float32)
    latent = latent / total
    high = latent.astype(jnp.bfloat16)
    low = (latent - high.astype(jnp.float32)).astype(jnp.bfloat16)
    for h in range(heads):
        mine = slice(h * tokens, (h + 1) * tokens)
        value = dot(high[mine, :], w_ref[h]) + dot(low[mine, :], w_ref[h])
        out_ref[:, h, :] = value


def finish(pieces, own, draft_latent, draft_rope, tree, w_value, tokens, heads):
    vmem = pl.BlockSpec(memory_space=pltpu.VMEM)
    return pl.pallas_call(
        functools.partial(finish_kernel, tokens, heads),
        out_shape=jax.ShapeDtypeStruct((tokens, heads, VDIM), jnp.float32),
        in_specs=[vmem] * 6,
        out_specs=vmem,
        name="finish",
    )(pieces, own, draft_latent, draft_rope, tree, w_value)


def ring(n, shift):
    return [(i, (i + shift) % n) for i in range(n)]


def shards(
    q_latent,
    q_rope,
    cache_latent,
    cache_rope,
    draft_latent,
    draft_rope,
    ancestors,
    valid_length,
    accepted,
    w_value,
):
    tokens, heads = q_latent.shape[:2]
    rows = cache_latent.shape[0]
    nx, nseq = lax.axis_size("x"), lax.axis_size(SEQ)
    x, core = lax.axis_index("x"), lax.axis_index("core")

    lat = q_latent.reshape(tokens, heads, 4, LANES).transpose(2, 1, 0, 3).reshape(4 * ROWS, LANES)
    rot = q_rope.transpose(2, 0, 1).reshape(ROWS, ROPE)
    rot = jnp.concatenate([rot[: ROWS // 2], rot[ROWS // 2 :]], axis=1)
    own_q = jnp.concatenate([lat, rot], axis=0)
    queries = lax.all_to_all(
        jnp.broadcast_to(own_q[None], (nseq, Q_ROWS, LANES)), SEQ, 0, 0, tiled=True
    )

    own = jnp.concatenate([cache_latent, cache_rope], axis=0)
    half = own.shape[0] // 2
    left = lax.ppermute(own, "x", ring(nx, 1))
    right = lax.ppermute(own, "x", ring(nx, nx - 1))
    far_top = lax.ppermute(left[:half], "x", ring(nx, 1))
    far_low = lax.ppermute(right[half:], "x", ring(nx, nx - 1))
    far = jnp.concatenate([far_top, far_low], axis=0)
    mine = (own, left, right, far)
    chunks = mine + tuple(lax.ppermute(a, "core", ring(2, 1)) for a in mine)
    offset = jnp.array([0, nx - 1, 1, 2] * 2, jnp.int32)
    other = jnp.array([0] * 4 + [1] * 4, jnp.int32)
    position = lax.axis_index(SEQ) * (nx * 2) + ((x + offset) % nx) * 2 + (core + other) % 2
    limits = valid_length - position * rows

    pieces = attend(limits, queries, chunks)
    pieces = lax.all_to_all(pieces, SEQ, 0, 0, tiled=True)
    blk = x * 2 + core
    tree = lax.dynamic_slice_in_dim(ancestors, blk * tokens, tokens, 0)
    attended = finish(pieces, own_q, draft_latent, draft_rope, tree, w_value, tokens, heads)
    count = jnp.broadcast_to(jnp.sum(accepted)[None], (nx * 2,))
    accepted_total = jnp.sum(lax.all_to_all(count, BLK, 0, 0, tiled=True))
    return (attended.astype(jnp.bfloat16), accepted_total)


def solution(mesh):
    finer = Mesh(mesh.devices.reshape(8, 4, 4, 2), SEQ + BLK)
    return jax.shard_map(
        shards,
        mesh=finer,
        in_specs=(
            P(BLK, SEQ, None),
            P(BLK, None, SEQ),
            P(SEQ + BLK, None),
            P(None, SEQ + BLK),
            P(),
            P(),
            P(),
            P(),
            P(BLK),
            P(SEQ, None, None),
        ),
        out_specs=(P(BLK, SEQ, None), P()),
        check_vma=False,
    )
```

```python
import functools
import math

import jax
import jax.numpy as jnp
from jax import lax
from jax.experimental import pallas as pl
from jax.experimental.pallas import tpu as pltpu
from jax.sharding import Mesh
from jax.sharding import PartitionSpec as P

ROPE = 64
VDIM = 128
LATENT = 512
LANES = 128
SEQ = ("z", "y")
BLK = ("x", "core")
NEG = -1e30
SCALE2 = (VDIM + ROPE) ** -0.5 * math.log2(math.e)

ROWS = 32
Q_ROWS = 144
O_ROWS = 136
OWNERS = 8
EXTRA = 8
BLOCK = OWNERS * ROWS


def dot(a, b, contract=((1,), (0,))):
    return lax.dot_general(a, b, (contract, ((), ())), preferred_element_type=jnp.float32)


def three_parts(value):
    high = value.astype(jnp.bfloat16)
    rest = value - high.astype(jnp.float32)
    middle = rest.astype(jnp.bfloat16)
    low = (rest - middle.astype(jnp.float32)).astype(jnp.bfloat16)
    return high, middle, low


def attend_kernel(n_queries, n_chunks, *refs):
    q_refs, chunks = refs[:n_queries], refs[n_queries : n_queries + n_chunks]
    out_ref, count_ref, query, query_rope, scores = refs[n_queries + n_chunks :]
    rows = LATENT
    lane = lax.broadcasted_iota(jnp.int32, (BLOCK, LANES), 1)
    query_rope[...] = jnp.where(lane == ROPE, 1.0, 0.0).astype(jnp.bfloat16)
    own_lane = lax.broadcasted_iota(jnp.int32, (ROWS, LANES), 1)
    own_row = lax.broadcasted_iota(jnp.int32, (ROWS, LANES), 0)
    count = jnp.zeros((EXTRA, LANES), jnp.float32)
    for c in range(n_chunks):
        count = count + chunks[c][rows + ROPE :, :LANES].astype(jnp.float32)
    count_ref[...] = count
    owners = [q_ref.at[i] for q_ref in q_refs for i in range(q_ref.shape[0])]
    for i in range(OWNERS):
        for j in range(4):
            query[i * ROWS : (i + 1) * ROWS, j * LANES : (j + 1) * LANES] = owners[i][
                j * ROWS : (j + 1) * ROWS, :
            ]
        both = owners[i][4 * ROWS :, :]
        query_rope[i * ROWS : i * ROWS + 16, :ROPE] = both[:, :ROPE]
        query_rope[i * ROWS + 16 : (i + 1) * ROWS, :ROPE] = both[:, ROPE:]
    peak = None
    for c in range(n_chunks):
        here = slice(c * rows, (c + 1) * rows)
        s = dot(query[...], chunks[c][:rows, :], ((1,), (1,)))
        s = s + dot(query_rope[:, : ROPE + EXTRA], chunks[c][rows:, :])
        scores[:, here] = s
        for j in range(rows // LANES):
            part = s[:, j * LANES : (j + 1) * LANES]
            peak = part if peak is None else jnp.maximum(peak, part)
    peak = jnp.max(peak, axis=1, keepdims=True)
    total = jnp.zeros((BLOCK, LANES), jnp.float32)
    latent = jnp.zeros((BLOCK, LATENT), jnp.float32)
    for c in range(n_chunks):
        here = slice(c * rows, (c + 1) * rows)
        p = jnp.exp2((scores[:, here] - peak) * SCALE2)
        for j in range(rows // LANES):
            total = total + p[:, j * LANES : (j + 1) * LANES]
        latent = latent + dot(p.astype(jnp.bfloat16), chunks[c][:rows, :])
    total = jnp.sum(total, axis=1, keepdims=True)
    latent = (latent * (1.0 / total)).astype(jnp.bfloat16)
    lse = peak * SCALE2 + jnp.log2(total)
    for i in range(OWNERS):
        mine = slice(i * ROWS, (i + 1) * ROWS)
        for j in range(4):
            out_ref[i, j * ROWS : (j + 1) * ROWS, :] = latent[mine, j * LANES : (j + 1) * LANES]
        line = jnp.where(own_lane == own_row, lse[mine, :], 0.0)
        out_ref[i, 4 * ROWS :, :] = lines_of(jnp.sum(line, axis=0, keepdims=True))


def lines_of(line):
    parts = [p.astype(jnp.float32) for p in three_parts(line)]
    pad = jnp.zeros((EXTRA - 3, LANES), jnp.float32)
    return jnp.concatenate(parts + [pad], axis=0).astype(jnp.bfloat16)


def attend(queries, chunks):
    vmem = pl.BlockSpec(memory_space=pltpu.VMEM)
    n = len(chunks)
    return pl.pallas_call(
        functools.partial(attend_kernel, len(queries), n),
        out_shape=(
            jax.ShapeDtypeStruct((OWNERS, O_ROWS, LANES), jnp.bfloat16),
            jax.ShapeDtypeStruct((EXTRA, LANES), jnp.float32),
        ),
        in_specs=[vmem] * (len(queries) + n),
        out_specs=(vmem, vmem),
        scratch_shapes=[
            pltpu.VMEM((BLOCK, LATENT), jnp.bfloat16),
            pltpu.VMEM((BLOCK, LANES), jnp.bfloat16),
            pltpu.VMEM((BLOCK, n * LATENT), jnp.float32),
        ],
        compiler_params=pltpu.CompilerParams(vmem_limit_bytes=12 * 2**20),
        cost_estimate=pl.CostEstimate(
            flops=BLOCK * n * LATENT * 2 * 1280, bytes_accessed=2**20, transcendentals=0
        ),
        name="attend",
    )(*queries, *chunks)


def merge_kernel(*refs):
    pieces, out_ref = refs[:-1], refs[-1]
    own_lane = lax.broadcasted_iota(jnp.int32, (ROWS, LANES), 1)
    diagonal = own_lane == lax.broadcasted_iota(jnp.int32, (ROWS, LANES), 0)
    for i in range(out_ref.shape[0]):
        lses = []
        for piece in pieces:
            parts = piece[i, 4 * ROWS :, :].astype(jnp.float32)
            lses.append(parts[0:1, :] + parts[1:2, :] + parts[2:3, :])
        peak = functools.reduce(jnp.maximum, lses)
        shares = [jnp.exp2(lse - peak) for lse in lses]
        total = sum(shares[1:], shares[0])
        out_ref[i, 4 * ROWS :, :] = lines_of(peak + jnp.log2(total))
        shares = [
            jnp.sum(jnp.where(diagonal, share / total, 0.0), axis=1, keepdims=True)
            for share in shares
        ]
        for j in range(4):
            mine = slice(j * ROWS, (j + 1) * ROWS)
            latent = sum(p[i, mine, :].astype(jnp.float32) * s for p, s in zip(pieces, shares))
            out_ref[i, mine, :] = latent.astype(jnp.bfloat16)


def merge(pieces):
    vmem = pl.BlockSpec(memory_space=pltpu.VMEM)
    return pl.pallas_call(
        merge_kernel,
        out_shape=jax.ShapeDtypeStruct(pieces[0].shape, pieces[0].dtype),
        in_specs=[vmem] * len(pieces),
        out_specs=vmem,
        compiler_params=pltpu.CompilerParams(vmem_limit_bytes=8 * 2**20),
        name="merge",
    )(*pieces)


def pack_query_kernel(lat_ref, rope_ref, out_ref, packed):
    tokens, heads = lat_ref.shape[:2]
    for t in range(tokens):
        lat = lat_ref[t].astype(jnp.float32)
        for j in range(4):
            first = j * ROWS + t * heads
            packed[first : first + heads, :] = lat[:, j * LANES : (j + 1) * LANES]
        first = 4 * ROWS + (t % (tokens // 2)) * heads
        side = (t // (tokens // 2)) * ROPE
        packed[first : first + heads, side : side + ROPE] = rope_ref[t].astype(jnp.float32)
    block = packed[...].astype(jnp.bfloat16)
    for i in range(out_ref.shape[0]):
        out_ref[i] = block


def pack_query(q_latent, q_rope, copies):
    vmem = pl.BlockSpec(memory_space=pltpu.VMEM)
    return pl.pallas_call(
        pack_query_kernel,
        out_shape=jax.ShapeDtypeStruct((copies, Q_ROWS, LANES), jnp.bfloat16),
        in_specs=[vmem] * 2,
        out_specs=vmem,
        scratch_shapes=[pltpu.VMEM((Q_ROWS, LANES), jnp.float32)],
        compiler_params=pltpu.CompilerParams(vmem_limit_bytes=8 * 2**20),
        name="pack_query",
    )(q_latent, q_rope)


def pack_cache_kernel(valid_ref, accepted_ref, lat_ref, rope_ref, out_ref):
    limit = valid_ref[0] - lax.axis_index(SEQ + BLK) * LATENT
    count = sum(accepted_ref[i] for i in range(accepted_ref.shape[0]))
    out_ref[:LATENT, :] = lat_ref[...]
    out_ref[LATENT : LATENT + ROPE, :] = rope_ref[...]
    lane = lax.broadcasted_iota(jnp.int32, (EXTRA, LATENT), 1)
    row = lax.broadcasted_iota(jnp.int32, (EXTRA, LATENT), 0)
    dead = jnp.where((row == 0) & (lane >= limit), NEG, 0.0)
    extra = jnp.where(row == 1, count.astype(jnp.float32), dead)
    out_ref[LATENT + ROPE :, :] = extra.astype(jnp.bfloat16)


def pack_cache(valid_length, accepted, cache_latent, cache_rope):
    vmem = pl.BlockSpec(memory_space=pltpu.VMEM)
    smem = pl.BlockSpec(memory_space=pltpu.SMEM)
    return pl.pallas_call(
        pack_cache_kernel,
        out_shape=jax.ShapeDtypeStruct((LATENT + ROPE + EXTRA, LATENT), jnp.bfloat16),
        in_specs=[smem, smem, vmem, vmem],
        out_specs=vmem,
        compiler_params=pltpu.CompilerParams(vmem_limit_bytes=8 * 2**20),
        name="pack_cache",
    )(valid_length.reshape(1), accepted, cache_latent, cache_rope)


def finish_kernel(tokens, heads, pieces_ref, q_ref, d_lat_ref, d_rope_ref, tree_ref, w_ref, out_ref):
    n = pieces_ref.shape[0]
    parts = pieces_ref[:, 4 * ROWS :, :].astype(jnp.float32)
    lse = parts[:, 0, :] + parts[:, 1, :] + parts[:, 2, :]
    query = jnp.concatenate([q_ref[j * ROWS : (j + 1) * ROWS, :] for j in range(4)], axis=1)
    both = q_ref[4 * ROWS :, :]
    query_rope = jnp.concatenate([both[:, :ROPE], both[:, ROPE:]], axis=0)
    draft = d_lat_ref[...]
    score = dot(query, draft, ((1,), (1,))) + dot(query_rope, d_rope_ref[...])
    score = jnp.where(tree_ref[...] == 1, score * SCALE2, NEG)
    draft_peak = jnp.max(score, axis=1, keepdims=True)
    own_lane = lax.broadcasted_iota(jnp.int32, (ROWS, LANES), 1)
    own_row = lax.broadcasted_iota(jnp.int32, (ROWS, LANES), 0)
    diagonal = own_lane == own_row

    def to_rows(line):
        return jnp.sum(jnp.where(diagonal, line, 0.0), axis=1, keepdims=True)

    cache_peak = to_rows(jnp.max(lse, axis=0, keepdims=True))
    peak = jnp.maximum(cache_peak, draft_peak)
    weight = jnp.exp2(score - peak)
    total = jnp.sum(weight, axis=1, keepdims=True)
    latent = dot(weight.astype(jnp.bfloat16), draft)
    for i in range(n):
        share = jnp.exp2(to_rows(lse[i : i + 1, :]) - peak)
        total = total + share
        piece = jnp.concatenate(
            [pieces_ref[i, j * ROWS : (j + 1) * ROWS, :] for j in range(4)], axis=1
        )
        latent = latent + share * piece.astype(jnp.float32)
    latent = latent / total
    high = latent.astype(jnp.bfloat16)
    low = (latent - high.astype(jnp.float32)).astype(jnp.bfloat16)
    head = lax.broadcasted_iota(jnp.int32, (ROWS, VDIM), 0) % heads
    value = jnp.zeros((ROWS, VDIM), jnp.float32)
    for h in range(heads):
        value = jnp.where(head == h, dot(high, w_ref[h]) + dot(low, w_ref[h]), value)
    for t in range(tokens):
        out_ref[t] = value[t * heads : (t + 1) * heads, :].astype(out_ref.dtype)


def finish(pieces, own, draft_latent, draft_rope, tree, w_value, tokens, heads):
    vmem = pl.BlockSpec(memory_space=pltpu.VMEM)
    return pl.pallas_call(
        functools.partial(finish_kernel, tokens, heads),
        out_shape=jax.ShapeDtypeStruct((tokens, heads, VDIM), jnp.bfloat16),
        in_specs=[vmem] * 6,
        out_specs=vmem,
        compiler_params=pltpu.CompilerParams(vmem_limit_bytes=8 * 2**20),
        name="finish",
    )(pieces, own, draft_latent, draft_rope, tree, w_value)


def both_ways(n, step):
    return [
        (i * 2 + core, (i + (step if core == 0 else -step)) % n * 2 + core)
        for i in range(n)
        for core in range(2)
    ]


def shift(value, axis, step):
    return lax.ppermute(value, (axis, "core"), both_ways(lax.axis_size(axis), step))


def across(value, axis):
    n = lax.axis_size(axis)
    return lax.ppermute(value, axis, [(i, (i + n // 2) % n) for i in range(n)])


def other_core(value):
    return lax.ppermute(value, "core", [(0, 1), (1, 0)])


def shards(
    q_latent,
    q_rope,
    cache_latent,
    cache_rope,
    draft_latent,
    draft_rope,
    ancestors,
    valid_length,
    accepted,
    w_value,
):
    tokens, heads = q_latent.shape[:2]
    nz = lax.axis_size("z")

    packed = pack_query(q_latent, q_rope.transpose(0, 2, 1), nz)
    own = pack_cache(valid_length, accepted, cache_latent, cache_rope)
    ahead = shift(own, "x", 1)
    behind = shift(own, "x", -1)
    far = shift(ahead, "x", 1)
    near = lax.all_to_all(packed, "z", 0, 0, tiled=True)
    q_far = across(near, "y")
    q_ahead = shift(near, "y", 1)
    q_behind = shift(near, "y", -1)
    mine = (own, ahead, behind, far)
    chunks = list(mine)
    for chunk in mine:
        chunks.append(other_core(chunk))

    part_far, counts = attend((q_far,), chunks)
    part_ahead, _ = attend((q_ahead,), chunks)
    part_behind, _ = attend((q_behind,), chunks)
    part_near, _ = attend((near,), chunks)
    from_far = across(part_far, "y")
    from_ahead = shift(part_ahead, "y", -1)
    from_behind = shift(part_behind, "y", 1)
    pieces = merge((part_near, from_far, from_ahead, from_behind))
    pieces = lax.all_to_all(pieces, "z", 0, 0, tiled=True)
    tree = lax.dynamic_slice_in_dim(ancestors, lax.axis_index(BLK) * tokens, tokens, 0)
    tree = jnp.repeat(tree, heads, axis=0)
    attended = finish(pieces, packed[0], draft_latent, draft_rope, tree, w_value, tokens, heads)
    return (attended, counts[1, 0].astype(jnp.int32))


def solution(mesh):
    finer = Mesh(mesh.devices.reshape(8, 4, 4, 2), SEQ + BLK)

    return jax.shard_map(
        shards,
        mesh=finer,
        in_specs=(
            P(BLK, SEQ, None),
            P(BLK, None, SEQ),
            P(SEQ + BLK, None),
            P(None, SEQ + BLK),
            P(),
            P(),
            P(),
            P(),
            P(BLK),
            P(SEQ, None, None),
        ),
        out_specs=(P(BLK, SEQ, None), P()),
        check_vma=False,
    )
```

```python
import functools
import math

import jax
import jax.numpy as jnp
from jax import lax
from jax.experimental import pallas as pl
from jax.experimental.pallas import tpu as pltpu
from jax.sharding import Mesh
from jax.sharding import PartitionSpec as P

ROPE = 64
VDIM = 128
LATENT = 512
LANES = 128
SEQ = ("z", "y")
BLK = ("x", "core")
NEG = -1e30
SCALE2 = (VDIM + ROPE) ** -0.5 * math.log2(math.e)

ROWS = 32
Q_ROWS = 144
O_ROWS = 136
OWNERS = 8
EXTRA = 8
BLOCK = OWNERS * ROWS


def dot(a, b, contract=((1,), (0,))):
    return lax.dot_general(a, b, (contract, ((), ())), preferred_element_type=jnp.float32)


def three_parts(value):
    high = value.astype(jnp.bfloat16)
    rest = value - high.astype(jnp.float32)
    middle = rest.astype(jnp.bfloat16)
    low = (rest - middle.astype(jnp.float32)).astype(jnp.bfloat16)
    return high, middle, low


def attend_kernel(n_queries, n_chunks, counted, *refs):
    q_refs, chunks = refs[:n_queries], refs[n_queries : n_queries + n_chunks]
    out_ref = refs[n_queries + n_chunks]
    query, query_rope, scores = refs[-3:]
    rows = LATENT
    lane = lax.broadcasted_iota(jnp.int32, (BLOCK, LANES), 1)
    query_rope[...] = jnp.where(lane == ROPE, 1.0, 0.0).astype(jnp.bfloat16)
    own_lane = lax.broadcasted_iota(jnp.int32, (ROWS, LANES), 1)
    own_row = lax.broadcasted_iota(jnp.int32, (ROWS, LANES), 0)
    if counted:
        count = jnp.zeros((EXTRA, LANES), jnp.float32)
        for c in range(n_chunks):
            count = count + chunks[c][rows + ROPE :, :LANES].astype(jnp.float32)
        refs[n_queries + n_chunks + 1][...] = count
    owners = [q_ref.at[i] for q_ref in q_refs for i in range(q_ref.shape[0])]
    for i in range(OWNERS):
        for j in range(4):
            query[i * ROWS : (i + 1) * ROWS, j * LANES : (j + 1) * LANES] = owners[i][
                j * ROWS : (j + 1) * ROWS, :
            ]
        both = owners[i][4 * ROWS :, :]
        query_rope[i * ROWS : i * ROWS + 16, :ROPE] = both[:, :ROPE]
        query_rope[i * ROWS + 16 : (i + 1) * ROWS, :ROPE] = both[:, ROPE:]
    peak = None
    for c in range(n_chunks):
        here = slice(c * rows, (c + 1) * rows)
        s = dot(query[...], chunks[c][:rows, :], ((1,), (1,)))
        s = s + dot(query_rope[:, : ROPE + EXTRA], chunks[c][rows:, :])
        scores[:, here] = s
        for j in range(rows // LANES):
            part = s[:, j * LANES : (j + 1) * LANES]
            peak = part if peak is None else jnp.maximum(peak, part)
    peak = jnp.max(peak, axis=1, keepdims=True)
    total = jnp.zeros((BLOCK, LANES), jnp.float32)
    latent = jnp.zeros((BLOCK, LATENT), jnp.float32)
    for c in range(n_chunks):
        here = slice(c * rows, (c + 1) * rows)
        p = jnp.exp2((scores[:, here] - peak) * SCALE2)
        for j in range(rows // LANES):
            total = total + p[:, j * LANES : (j + 1) * LANES]
        latent = latent + dot(p.astype(jnp.bfloat16), chunks[c][:rows, :])
    total = jnp.sum(total, axis=1, keepdims=True)
    latent = (latent * (1.0 / total)).astype(jnp.bfloat16)
    lse = peak * SCALE2 + jnp.log2(total)
    for i in range(OWNERS):
        mine = slice(i * ROWS, (i + 1) * ROWS)
        for j in range(4):
            out_ref[i, j * ROWS : (j + 1) * ROWS, :] = latent[mine, j * LANES : (j + 1) * LANES]
        line = jnp.where(own_lane == own_row, lse[mine, :], 0.0)
        out_ref[i, 4 * ROWS :, :] = lines_of(jnp.sum(line, axis=0, keepdims=True))


def lines_of(line):
    parts = [p.astype(jnp.float32) for p in three_parts(line)]
    pad = jnp.zeros((EXTRA - 3, LANES), jnp.float32)
    return jnp.concatenate(parts + [pad], axis=0).astype(jnp.bfloat16)


def attend(queries, chunks, counted=False):
    vmem = pl.BlockSpec(memory_space=pltpu.VMEM)
    n = len(chunks)
    return pl.pallas_call(
        functools.partial(attend_kernel, len(queries), n, counted),
        out_shape=[
            jax.ShapeDtypeStruct((OWNERS, O_ROWS, LANES), jnp.bfloat16),
            jax.ShapeDtypeStruct((EXTRA, LANES), jnp.float32),
        ][: 2 if counted else 1],
        in_specs=[vmem] * (len(queries) + n),
        out_specs=[vmem] * (2 if counted else 1),
        scratch_shapes=[
            pltpu.VMEM((BLOCK, LATENT), jnp.bfloat16),
            pltpu.VMEM((BLOCK, LANES), jnp.bfloat16),
            pltpu.VMEM((BLOCK, n * LATENT), jnp.float32),
        ],
        compiler_params=pltpu.CompilerParams(vmem_limit_bytes=12 * 2**20),
        cost_estimate=pl.CostEstimate(
            flops=BLOCK * n * LATENT * 2 * 1280, bytes_accessed=2**20, transcendentals=0
        ),
        name="attend",
    )(*queries, *chunks)


def merge_kernel(n_pieces, *refs):
    pieces, outs = refs[:n_pieces], refs[n_pieces:]
    place = lax.axis_index("z")
    n = pieces[0].shape[0]
    own_lane = lax.broadcasted_iota(jnp.int32, (ROWS, LANES), 1)
    diagonal = own_lane == lax.broadcasted_iota(jnp.int32, (ROWS, LANES), 0)
    owners = [lax.rem(place - 2 * (i // 2) + n, n) for i in range(n)]
    owners = [z + (i % 2) * (1 - 2 * lax.rem(z, 2)) for i, z in enumerate(owners)]
    blocks = [outs[0].at[z] for z in owners]
    for i, out in enumerate(blocks):
        lses = []
        for piece in pieces:
            parts = piece[i, 4 * ROWS :, :].astype(jnp.float32)
            lses.append(parts[0:1, :] + parts[1:2, :] + parts[2:3, :])
        peak = functools.reduce(jnp.maximum, lses)
        shares = [jnp.exp2(lse - peak) for lse in lses]
        total = sum(shares[1:], shares[0])
        out[4 * ROWS :, :] = lines_of(peak + jnp.log2(total))
        shares = [
            jnp.sum(jnp.where(diagonal, share / total, 0.0), axis=1, keepdims=True)
            for share in shares
        ]
        for j in range(4):
            mine = slice(j * ROWS, (j + 1) * ROWS)
            latent = sum(p[i, mine, :].astype(jnp.float32) * s for p, s in zip(pieces, shares))
            out[mine, :] = latent.astype(jnp.bfloat16)


def merge(pieces, groups):
    vmem = pl.BlockSpec(memory_space=pltpu.VMEM)
    n, rest = pieces[0].shape[0], pieces[0].shape[1:]
    return pl.pallas_call(
        functools.partial(merge_kernel, len(pieces)),
        out_shape=[jax.ShapeDtypeStruct((n // groups, *rest), jnp.bfloat16)] * groups,
        in_specs=[vmem] * len(pieces),
        out_specs=[vmem] * groups,
        compiler_params=pltpu.CompilerParams(vmem_limit_bytes=8 * 2**20),
        name="merge",
    )(*pieces)


def pack_query_kernel(lat_ref, rope_ref, out_ref, packed):
    tokens, heads = lat_ref.shape[:2]
    for t in range(tokens):
        lat = lat_ref[t].astype(jnp.float32)
        for j in range(4):
            first = j * ROWS + t * heads
            packed[first : first + heads, :] = lat[:, j * LANES : (j + 1) * LANES]
        first = 4 * ROWS + (t % (tokens // 2)) * heads
        side = (t // (tokens // 2)) * ROPE
        packed[first : first + heads, side : side + ROPE] = rope_ref[t].astype(jnp.float32)
    block = packed[...].astype(jnp.bfloat16)
    for i in range(out_ref.shape[0]):
        out_ref[i] = block


def pack_query(q_latent, q_rope, copies):
    vmem = pl.BlockSpec(memory_space=pltpu.VMEM)
    return pl.pallas_call(
        pack_query_kernel,
        out_shape=jax.ShapeDtypeStruct((copies, Q_ROWS, LANES), jnp.bfloat16),
        in_specs=[vmem] * 2,
        out_specs=vmem,
        scratch_shapes=[pltpu.VMEM((Q_ROWS, LANES), jnp.float32)],
        compiler_params=pltpu.CompilerParams(vmem_limit_bytes=8 * 2**20),
        name="pack_query",
    )(q_latent, q_rope)


def pack_cache_kernel(valid_ref, accepted_ref, lat, rope, out_ref, sems):
    copies = [
        pltpu.make_async_copy(lat, out_ref.at[:LATENT], sems.at[0]),
        pltpu.make_async_copy(rope, out_ref.at[LATENT : LATENT + ROPE], sems.at[1]),
    ]
    for copy in copies:
        copy.start()
    limit = valid_ref[0] - lax.axis_index(SEQ + BLK) * LATENT
    count = sum(accepted_ref[i] for i in range(accepted_ref.shape[0]))
    lane = lax.broadcasted_iota(jnp.int32, (EXTRA, LATENT), 1)
    row = lax.broadcasted_iota(jnp.int32, (EXTRA, LATENT), 0)
    dead = jnp.where((row == 0) & (lane >= limit), NEG, 0.0)
    extra = jnp.where(row == 1, count.astype(jnp.float32), dead)
    out_ref[LATENT + ROPE :, :] = extra.astype(jnp.bfloat16)
    copies[0].wait()
    copies[1].wait()


def pack_cache(valid_length, accepted, cache_latent, cache_rope):
    return pl.pallas_call(
        pack_cache_kernel,
        out_shape=jax.ShapeDtypeStruct((LATENT + ROPE + EXTRA, LATENT), jnp.bfloat16),
        in_specs=[pl.BlockSpec(memory_space=pltpu.SMEM)] * 2
        + [pl.BlockSpec(memory_space=pltpu.HBM)] * 2,
        out_specs=pl.BlockSpec(memory_space=pltpu.VMEM),
        scratch_shapes=[pltpu.SemaphoreType.DMA((2,))],
        compiler_params=pltpu.CompilerParams(vmem_limit_bytes=60 * 1024 * 2**10 - 660 * 2**10),
        name="pack_cache",
    )(valid_length.reshape(1), accepted, cache_latent, cache_rope)


def finish_kernel(tokens, heads, pieces_ref, q_ref, d_lat_ref, d_rope_ref, tree_ref, w_ref, out_ref):
    pieces = [pieces_ref.at[i] for i in range(pieces_ref.shape[0])]
    lses = []
    for piece in pieces:
        parts = piece[4 * ROWS :, :].astype(jnp.float32)
        lses.append(parts[0:1, :] + parts[1:2, :] + parts[2:3, :])
    q_ref = q_ref.at[0]
    query = jnp.concatenate([q_ref[j * ROWS : (j + 1) * ROWS, :] for j in range(4)], axis=1)
    both = q_ref[4 * ROWS :, :]
    query_rope = jnp.concatenate([both[:, :ROPE], both[:, ROPE:]], axis=0)
    draft = d_lat_ref[...]
    score = dot(query, draft, ((1,), (1,))) + dot(query_rope, d_rope_ref[...])
    score = jnp.where(tree_ref[...] == 1, score * SCALE2, NEG)
    draft_peak = jnp.max(score, axis=1, keepdims=True)
    own_lane = lax.broadcasted_iota(jnp.int32, (ROWS, LANES), 1)
    own_row = lax.broadcasted_iota(jnp.int32, (ROWS, LANES), 0)
    diagonal = own_lane == own_row

    def to_rows(line):
        return jnp.sum(jnp.where(diagonal, line, 0.0), axis=1, keepdims=True)

    cache_peak = to_rows(functools.reduce(jnp.maximum, lses))
    peak = jnp.maximum(cache_peak, draft_peak)
    weight = jnp.exp2(score - peak)
    total = jnp.sum(weight, axis=1, keepdims=True)
    latent = dot(weight.astype(jnp.bfloat16), draft)
    for piece, lse in zip(pieces, lses):
        share = jnp.exp2(to_rows(lse) - peak)
        total = total + share
        piece = jnp.concatenate([piece[j * ROWS : (j + 1) * ROWS, :] for j in range(4)], axis=1)
        latent = latent + share * piece.astype(jnp.float32)
    latent = latent / total
    high = latent.astype(jnp.bfloat16)
    low = (latent - high.astype(jnp.float32)).astype(jnp.bfloat16)
    head = lax.broadcasted_iota(jnp.int32, (ROWS, VDIM), 0) % heads
    value = jnp.zeros((ROWS, VDIM), jnp.float32)
    for h in range(heads):
        value = jnp.where(head == h, dot(high, w_ref[h]) + dot(low, w_ref[h]), value)
    for t in range(tokens):
        out_ref[t] = value[t * heads : (t + 1) * heads, :].astype(out_ref.dtype)


def finish(pieces, own, draft_latent, draft_rope, tree, w_value, tokens, heads):
    vmem = pl.BlockSpec(memory_space=pltpu.VMEM)
    return pl.pallas_call(
        functools.partial(finish_kernel, tokens, heads),
        out_shape=jax.ShapeDtypeStruct((tokens, heads, VDIM), jnp.bfloat16),
        in_specs=[vmem] * 6,
        out_specs=vmem,
        compiler_params=pltpu.CompilerParams(vmem_limit_bytes=8 * 2**20),
        name="finish",
    )(pieces, own, draft_latent, draft_rope, tree, w_value)


def both_ways(n, step):
    return [
        (i * 2 + core, (i + (step if core == 0 else -step)) % n * 2 + core)
        for i in range(n)
        for core in range(2)
    ]


def shift(value, axis, step):
    return lax.ppermute(value, (axis, "core"), both_ways(lax.axis_size(axis), step))


def across(value, axis):
    n = lax.axis_size(axis)
    return lax.ppermute(value, axis, [(i, (i + n // 2) % n) for i in range(n)])


def pair(value, axis):
    return lax.ppermute(value, axis, [(i, i ^ 1) for i in range(lax.axis_size(axis))])


def rotate(value, axis, step):
    n = lax.axis_size(axis)
    return lax.ppermute(value, axis, [(i, (i + step) % n) for i in range(n)])


def other_core(value):
    return lax.ppermute(value, "core", [(0, 1), (1, 0)])


def shards(
    q_latent,
    q_rope,
    cache_latent,
    cache_rope,
    draft_latent,
    draft_rope,
    ancestors,
    valid_length,
    accepted,
    w_value,
):
    tokens, heads = q_latent.shape[:2]
    nz = lax.axis_size("z")

    packed = pack_query(q_latent, q_rope.transpose(0, 2, 1), 1)
    own = pack_cache(valid_length, accepted, cache_latent, cache_rope)
    ahead = shift(own, "x", 1)
    behind = shift(own, "x", -1)
    far = shift(ahead, "x", 1)
    near = jnp.concatenate([packed, pair(packed, "z")], axis=0)
    turned = [near]
    for step in range(2, nz, 2):
        turned.append(rotate(near, "z", step))
    near = jnp.concatenate(turned, axis=0)
    q_far = across(near, "y")
    q_ahead = shift(near, "y", 1)
    q_behind = shift(near, "y", -1)
    mine = (own, ahead, behind, far)
    chunks = list(mine)
    for chunk in mine:
        chunks.append(other_core(chunk))

    part_far, counts = attend((q_far,), chunks, counted=True)
    (part_ahead,) = attend((q_ahead,), chunks)
    (part_behind,) = attend((q_behind,), chunks)
    (part_near,) = attend((near,), chunks)
    from_far = across(part_far, "y")
    from_ahead = shift(part_ahead, "y", -1)
    from_behind = shift(part_behind, "y", 1)
    (pieces,) = merge((part_near, from_far, from_ahead, from_behind), 1)
    pieces = lax.all_to_all(pieces, "z", 0, 0, tiled=True)
    tree = lax.dynamic_slice_in_dim(ancestors, lax.axis_index(BLK) * tokens, tokens, 0)
    tree = jnp.repeat(tree, heads, axis=0)
    attended = finish(pieces, packed, draft_latent, draft_rope, tree, w_value, tokens, heads)
    return (attended, counts[1, 0].astype(jnp.int32))


def solution(mesh):
    finer = Mesh(mesh.devices.reshape(8, 4, 4, 2), SEQ + BLK)

    return jax.shard_map(
        shards,
        mesh=finer,
        in_specs=(
            P(BLK, SEQ, None),
            P(BLK, None, SEQ),
            P(SEQ + BLK, None),
            P(None, SEQ + BLK),
            P(),
            P(),
            P(),
            P(),
            P(BLK),
            P(SEQ, None, None),
        ),
        out_specs=(P(BLK, SEQ, None), P()),
        check_vma=False,
    )
```

```python
import functools
import math

import jax
import jax.numpy as jnp
from jax import lax
from jax.experimental import pallas as pl
from jax.experimental.pallas import tpu as pltpu
from jax.sharding import Mesh
from jax.sharding import PartitionSpec as P

ROPE = 64
VDIM = 128
LATENT = 512
LANES = 128
SEQ = ("z", "y")
BLK = ("x", "core")
NEG = -1e30
SCALE2 = (VDIM + ROPE) ** -0.5 * math.log2(math.e)

ROWS = 32
Q_ROWS = 144
O_ROWS = 136
OWNERS = 8
EXTRA = 8
BLOCK = OWNERS * ROWS


def dot(a, b, contract=((1,), (0,))):
    return lax.dot_general(a, b, (contract, ((), ())), preferred_element_type=jnp.float32)


def three_parts(value):
    high = value.astype(jnp.bfloat16)
    rest = value - high.astype(jnp.float32)
    middle = rest.astype(jnp.bfloat16)
    low = (rest - middle.astype(jnp.float32)).astype(jnp.bfloat16)
    return high, middle, low


def attend_kernel(n_queries, n_chunks, counted, *refs):
    q_refs, chunks = refs[:n_queries], refs[n_queries : n_queries + n_chunks]
    out_ref = refs[n_queries + n_chunks]
    query, query_rope, scores, weights = refs[-4:]
    rows = LATENT
    lane = lax.broadcasted_iota(jnp.int32, (BLOCK, LANES), 1)
    query_rope[...] = jnp.where(lane == ROPE, 1.0, 0.0).astype(jnp.bfloat16)
    own_lane = lax.broadcasted_iota(jnp.int32, (ROWS, LANES), 1)
    own_row = lax.broadcasted_iota(jnp.int32, (ROWS, LANES), 0)
    if counted:
        count = jnp.zeros((EXTRA, LANES), jnp.float32)
        for c in range(n_chunks):
            count = count + chunks[c][rows + ROPE :, :LANES].astype(jnp.float32)
        refs[n_queries + n_chunks + 1][...] = count
    owners = [q_ref.at[i] for q_ref in q_refs for i in range(q_ref.shape[0])]
    for i in range(OWNERS):
        for j in range(4):
            query[i * ROWS : (i + 1) * ROWS, j * LANES : (j + 1) * LANES] = owners[i][
                j * ROWS : (j + 1) * ROWS, :
            ]
        both = owners[i][4 * ROWS :, :]
        query_rope[i * ROWS : i * ROWS + 16, :ROPE] = both[:, :ROPE]
        query_rope[i * ROWS + 16 : (i + 1) * ROWS, :ROPE] = both[:, ROPE:]
    half = n_chunks // 2

    def score(c):
        s = dot(query[...], chunks[c][:rows, :], ((1,), (1,)))
        s = s + dot(query_rope[:, : ROPE + EXTRA], chunks[c][rows:, :])
        scores[:, c * rows : (c + 1) * rows] = s
        tiles = [s[:, j * LANES : (j + 1) * LANES] for j in range(rows // LANES)]
        return functools.reduce(jnp.maximum, tiles)

    def weigh(c, peak):
        p = jnp.exp2((scores[:, c * rows : (c + 1) * rows] - peak) * SCALE2)
        weights[:, c * rows : (c + 1) * rows] = p.astype(jnp.bfloat16)
        tiles = [p[:, j * LANES : (j + 1) * LANES] for j in range(rows // LANES)]
        return sum(tiles[1:], tiles[0])

    def value(c):
        return dot(weights[:, c * rows : (c + 1) * rows], chunks[c][:rows, :])

    peak_a = functools.reduce(jnp.maximum, [score(c) for c in range(half)])
    peak_a = jnp.max(peak_a, axis=1, keepdims=True)
    peak_b, total_a = None, None
    for c in range(half):
        part = score(half + c)
        peak_b = part if peak_b is None else jnp.maximum(peak_b, part)
        part = weigh(c, peak_a)
        total_a = part if total_a is None else total_a + part
    peak_b = jnp.max(peak_b, axis=1, keepdims=True)
    latent_a, total_b = None, None
    for c in range(half):
        part = value(c)
        latent_a = part if latent_a is None else latent_a + part
        part = weigh(half + c, peak_b)
        total_b = part if total_b is None else total_b + part
    latent_b = sum((value(c) for c in range(half + 1, n_chunks)), value(half))
    peak = jnp.maximum(peak_a, peak_b)
    keep_a = jnp.exp2((peak_a - peak) * SCALE2)
    keep_b = jnp.exp2((peak_b - peak) * SCALE2)
    total_a = jnp.sum(total_a, axis=1, keepdims=True) * keep_a
    total_b = jnp.sum(total_b, axis=1, keepdims=True) * keep_b
    total = total_a + total_b
    latent = latent_a * (keep_a / total) + latent_b * (keep_b / total)
    latent = latent.astype(jnp.bfloat16)
    lse = peak * SCALE2 + jnp.log2(total)
    for i in range(OWNERS):
        mine = slice(i * ROWS, (i + 1) * ROWS)
        for j in range(4):
            out_ref[i, j * ROWS : (j + 1) * ROWS, :] = latent[mine, j * LANES : (j + 1) * LANES]
        line = jnp.where(own_lane == own_row, lse[mine, :], 0.0)
        out_ref[i, 4 * ROWS :, :] = lines_of(jnp.sum(line, axis=0, keepdims=True))


def lines_of(line):
    parts = [p.astype(jnp.float32) for p in three_parts(line)]
    pad = jnp.zeros((EXTRA - 3, LANES), jnp.float32)
    return jnp.concatenate(parts + [pad], axis=0).astype(jnp.bfloat16)


def attend(queries, chunks, counted=False):
    vmem = pl.BlockSpec(memory_space=pltpu.VMEM)
    n = len(chunks)
    return pl.pallas_call(
        functools.partial(attend_kernel, len(queries), n, counted),
        out_shape=[
            jax.ShapeDtypeStruct((OWNERS, O_ROWS, LANES), jnp.bfloat16),
            jax.ShapeDtypeStruct((EXTRA, LANES), jnp.float32),
        ][: 2 if counted else 1],
        in_specs=[vmem] * (len(queries) + n),
        out_specs=[vmem] * (2 if counted else 1),
        scratch_shapes=[
            pltpu.VMEM((BLOCK, LATENT), jnp.bfloat16),
            pltpu.VMEM((BLOCK, LANES), jnp.bfloat16),
            pltpu.VMEM((BLOCK, n * LATENT), jnp.float32),
            pltpu.VMEM((BLOCK, n * LATENT), jnp.bfloat16),
        ],
        compiler_params=pltpu.CompilerParams(vmem_limit_bytes=14 * 2**20),
        cost_estimate=pl.CostEstimate(
            flops=BLOCK * n * LATENT * 2 * 1280, bytes_accessed=2**20, transcendentals=0
        ),
        name="attend",
    )(*queries, *chunks)


def merge_kernel(n_pieces, *refs):
    pieces, outs = refs[:n_pieces], refs[n_pieces:]
    place = lax.axis_index("z")
    n = pieces[0].shape[0]
    own_lane = lax.broadcasted_iota(jnp.int32, (ROWS, LANES), 1)
    diagonal = own_lane == lax.broadcasted_iota(jnp.int32, (ROWS, LANES), 0)
    owners = [lax.rem(place - 2 * (i // 2) + n, n) for i in range(n)]
    owners = [z + (i % 2) * (1 - 2 * lax.rem(z, 2)) for i, z in enumerate(owners)]
    blocks = [outs[0].at[z] for z in owners]
    for i, out in enumerate(blocks):
        lses = []
        for piece in pieces:
            parts = piece[i, 4 * ROWS :, :].astype(jnp.float32)
            lses.append(parts[0:1, :] + parts[1:2, :] + parts[2:3, :])
        peak = functools.reduce(jnp.maximum, lses)
        shares = [jnp.exp2(lse - peak) for lse in lses]
        total = sum(shares[1:], shares[0])
        out[4 * ROWS :, :] = lines_of(peak + jnp.log2(total))
        shares = [
            jnp.sum(jnp.where(diagonal, share / total, 0.0), axis=1, keepdims=True)
            for share in shares
        ]
        for j in range(4):
            mine = slice(j * ROWS, (j + 1) * ROWS)
            latent = sum(p[i, mine, :].astype(jnp.float32) * s for p, s in zip(pieces, shares))
            out[mine, :] = latent.astype(jnp.bfloat16)


def merge(pieces, groups):
    vmem = pl.BlockSpec(memory_space=pltpu.VMEM)
    n, rest = pieces[0].shape[0], pieces[0].shape[1:]
    return pl.pallas_call(
        functools.partial(merge_kernel, len(pieces)),
        out_shape=[jax.ShapeDtypeStruct((n // groups, *rest), jnp.bfloat16)] * groups,
        in_specs=[vmem] * len(pieces),
        out_specs=[vmem] * groups,
        compiler_params=pltpu.CompilerParams(vmem_limit_bytes=8 * 2**20),
        name="merge",
    )(*pieces)


def pack_query_kernel(lat_ref, rope_ref, out_ref, packed):
    tokens, heads = lat_ref.shape[:2]
    for t in range(tokens):
        lat = lat_ref[t].astype(jnp.float32)
        for j in range(4):
            first = j * ROWS + t * heads
            packed[first : first + heads, :] = lat[:, j * LANES : (j + 1) * LANES]
        first = 4 * ROWS + (t % (tokens // 2)) * heads
        side = (t // (tokens // 2)) * ROPE
        packed[first : first + heads, side : side + ROPE] = rope_ref[t].astype(jnp.float32)
    block = packed[...].astype(jnp.bfloat16)
    for i in range(out_ref.shape[0]):
        out_ref[i] = block


def pack_query(q_latent, q_rope, copies):
    vmem = pl.BlockSpec(memory_space=pltpu.VMEM)
    return pl.pallas_call(
        pack_query_kernel,
        out_shape=jax.ShapeDtypeStruct((copies, Q_ROWS, LANES), jnp.bfloat16),
        in_specs=[vmem] * 2,
        out_specs=vmem,
        scratch_shapes=[pltpu.VMEM((Q_ROWS, LANES), jnp.float32)],
        compiler_params=pltpu.CompilerParams(vmem_limit_bytes=8 * 2**20),
        name="pack_query",
    )(q_latent, q_rope)


def pack_cache_kernel(valid, accepted, lat, rope, out, packed, valid_ref, accepted_ref, sems):
    parts = 4
    step = LATENT // parts
    spans = [slice(i * step, (i + 1) * step) for i in range(parts)]
    loads = [
        pltpu.make_async_copy(lat.at[span], packed.at[span], sems.at[i])
        for i, span in enumerate(spans)
    ]
    last = slice(LATENT, LATENT + ROPE + EXTRA)
    rest = [
        pltpu.make_async_copy(rope, packed.at[LATENT : LATENT + ROPE], sems.at[parts]),
        pltpu.make_async_copy(valid, valid_ref, sems.at[parts + 1]),
        pltpu.make_async_copy(accepted, accepted_ref, sems.at[parts + 2]),
    ]
    stores = [
        pltpu.make_async_copy(packed.at[span], out.at[span], sems.at[parts + 3 + i])
        for i, span in enumerate(spans + [last])
    ]
    for copy in rest + loads:
        copy.start()
    for copy in rest:
        copy.wait()
    limit = valid_ref[0] - lax.axis_index(SEQ + BLK) * LATENT
    count = sum(accepted_ref[i] for i in range(accepted_ref.shape[0]))
    lane = lax.broadcasted_iota(jnp.int32, (EXTRA, LATENT), 1)
    row = lax.broadcasted_iota(jnp.int32, (EXTRA, LATENT), 0)
    dead = jnp.where((row == 0) & (lane >= limit), NEG, 0.0)
    extra = jnp.where(row == 1, count.astype(jnp.float32), dead)
    packed[LATENT + ROPE :, :] = extra.astype(jnp.bfloat16)
    for load, store in zip(loads, stores):
        load.wait()
        store.start()
    stores[-1].start()
    for store in stores:
        store.wait()


def pack_cache(valid_length, accepted, cache_latent, cache_rope):
    hbm = pl.BlockSpec(memory_space=pltpu.HBM)
    rows = LATENT + ROPE + EXTRA
    return pl.pallas_call(
        pack_cache_kernel,
        out_shape=jax.ShapeDtypeStruct((rows, LATENT), jnp.bfloat16),
        in_specs=[hbm] * 4,
        out_specs=hbm,
        scratch_shapes=[
            pltpu.VMEM((rows, LATENT), jnp.bfloat16),
            pltpu.SMEM((1,), jnp.int32),
            pltpu.SMEM(accepted.shape, jnp.int32),
            pltpu.SemaphoreType.DMA((12,)),
        ],
        compiler_params=pltpu.CompilerParams(vmem_limit_bytes=60 * 1024 * 2**10 - 660 * 2**10),
        name="pack_cache",
    )(valid_length.reshape(1), accepted, cache_latent, cache_rope)


def finish_kernel(tokens, heads, pieces_ref, q_ref, d_lat_ref, d_rope_ref, tree_ref, w_ref, out_ref):
    pieces = [pieces_ref.at[i] for i in range(pieces_ref.shape[0])]
    lses = []
    for piece in pieces:
        parts = piece[4 * ROWS :, :].astype(jnp.float32)
        lses.append(parts[0:1, :] + parts[1:2, :] + parts[2:3, :])
    q_ref = q_ref.at[0]
    query = jnp.concatenate([q_ref[j * ROWS : (j + 1) * ROWS, :] for j in range(4)], axis=1)
    both = q_ref[4 * ROWS :, :]
    query_rope = jnp.concatenate([both[:, :ROPE], both[:, ROPE:]], axis=0)
    draft = d_lat_ref[...]
    score = dot(query, draft, ((1,), (1,))) + dot(query_rope, d_rope_ref[...])
    score = jnp.where(tree_ref[...] == 1, score * SCALE2, NEG)
    draft_peak = jnp.max(score, axis=1, keepdims=True)
    own_lane = lax.broadcasted_iota(jnp.int32, (ROWS, LANES), 1)
    own_row = lax.broadcasted_iota(jnp.int32, (ROWS, LANES), 0)
    diagonal = own_lane == own_row

    def to_rows(line):
        return jnp.sum(jnp.where(diagonal, line, 0.0), axis=1, keepdims=True)

    cache_peak = to_rows(functools.reduce(jnp.maximum, lses))
    peak = jnp.maximum(cache_peak, draft_peak)
    weight = jnp.exp2(score - peak)
    total = jnp.sum(weight, axis=1, keepdims=True)
    latent = dot(weight.astype(jnp.bfloat16), draft)
    for piece, lse in zip(pieces, lses):
        share = jnp.exp2(to_rows(lse) - peak)
        total = total + share
        piece = jnp.concatenate([piece[j * ROWS : (j + 1) * ROWS, :] for j in range(4)], axis=1)
        latent = latent + share * piece.astype(jnp.float32)
    latent = latent / total
    high = latent.astype(jnp.bfloat16)
    low = (latent - high.astype(jnp.float32)).astype(jnp.bfloat16)
    head = lax.broadcasted_iota(jnp.int32, (ROWS, VDIM), 0) % heads
    value = jnp.zeros((ROWS, VDIM), jnp.float32)
    for h in range(heads):
        value = jnp.where(head == h, dot(high, w_ref[h]) + dot(low, w_ref[h]), value)
    for t in range(tokens):
        out_ref[t] = value[t * heads : (t + 1) * heads, :].astype(out_ref.dtype)


def finish(pieces, own, draft_latent, draft_rope, tree, w_value, tokens, heads):
    vmem = pl.BlockSpec(memory_space=pltpu.VMEM)
    return pl.pallas_call(
        functools.partial(finish_kernel, tokens, heads),
        out_shape=jax.ShapeDtypeStruct((tokens, heads, VDIM), jnp.bfloat16),
        in_specs=[vmem] * 6,
        out_specs=vmem,
        compiler_params=pltpu.CompilerParams(vmem_limit_bytes=8 * 2**20),
        name="finish",
    )(pieces, own, draft_latent, draft_rope, tree, w_value)


def both_ways(n, step):
    return [
        (i * 2 + core, (i + (step if core == 0 else -step)) % n * 2 + core)
        for i in range(n)
        for core in range(2)
    ]


def shift(value, axis, step):
    return lax.ppermute(value, (axis, "core"), both_ways(lax.axis_size(axis), step))


def across(value, axis):
    n = lax.axis_size(axis)
    return lax.ppermute(value, axis, [(i, (i + n // 2) % n) for i in range(n)])


def pair(value, axis):
    return lax.ppermute(value, axis, [(i, i ^ 1) for i in range(lax.axis_size(axis))])


def rotate(value, axis, step):
    n = lax.axis_size(axis)
    return lax.ppermute(value, axis, [(i, (i + step) % n) for i in range(n)])


def other_core(value):
    return lax.ppermute(value, "core", [(0, 1), (1, 0)])


def shards(
    q_latent,
    q_rope,
    cache_latent,
    cache_rope,
    draft_latent,
    draft_rope,
    ancestors,
    valid_length,
    accepted,
    w_value,
):
    tokens, heads = q_latent.shape[:2]
    nz = lax.axis_size("z")

    packed = pack_query(q_latent, q_rope.transpose(0, 2, 1), 1)
    own = pack_cache(valid_length, accepted, cache_latent, cache_rope)
    ahead = shift(own, "x", 1)
    behind = shift(own, "x", -1)
    far = shift(ahead, "x", 1)
    near = jnp.concatenate([packed, pair(packed, "z")], axis=0)
    turned = [near]
    for step in range(2, nz, 2):
        turned.append(rotate(near, "z", step))
    near = jnp.concatenate(turned, axis=0)
    q_far = across(near, "y")
    q_ahead = shift(near, "y", 1)
    q_behind = shift(near, "y", -1)
    mine = (own, ahead, behind, far)
    chunks = list(mine)
    for chunk in mine:
        chunks.append(other_core(chunk))

    part_far, counts = attend((q_far,), chunks, counted=True)
    (part_ahead,) = attend((q_ahead,), chunks)
    (part_behind,) = attend((q_behind,), chunks)
    (part_near,) = attend((near,), chunks)
    from_far = across(part_far, "y")
    from_ahead = shift(part_ahead, "y", -1)
    from_behind = shift(part_behind, "y", 1)
    (pieces,) = merge((part_near, from_far, from_ahead, from_behind), 1)
    pieces = lax.all_to_all(pieces, "z", 0, 0, tiled=True)
    tree = lax.dynamic_slice_in_dim(ancestors, lax.axis_index(BLK) * tokens, tokens, 0)
    tree = jnp.repeat(tree, heads, axis=0)
    attended = finish(pieces, packed, draft_latent, draft_rope, tree, w_value, tokens, heads)
    return (attended, counts[1, 0].astype(jnp.int32))


def solution(mesh):
    finer = Mesh(mesh.devices.reshape(8, 4, 4, 2), SEQ + BLK)

    return jax.shard_map(
        shards,
        mesh=finer,
        in_specs=(
            P(BLK, SEQ, None),
            P(BLK, None, SEQ),
            P(SEQ + BLK, None),
            P(None, SEQ + BLK),
            P(),
            P(),
            P(),
            P(),
            P(BLK),
            P(SEQ, None, None),
        ),
        out_specs=(P(BLK, SEQ, None), P()),
        check_vma=False,
    )
```

```python
import functools
import math

import jax
import jax.numpy as jnp
from jax import lax
from jax.experimental import pallas as pl
from jax.experimental.pallas import tpu as pltpu
from jax.sharding import Mesh
from jax.sharding import PartitionSpec as P

ROPE = 64
VDIM = 128
LATENT = 512
LANES = 128
SEQ = ("z", "y")
BLK = ("x", "core")
NEG = -1e30
SCALE2 = (VDIM + ROPE) ** -0.5 * math.log2(math.e)

ROWS = 32
Q_ROWS = 144
O_ROWS = 136
OWNERS = 8
EXTRA = 8
BLOCK = OWNERS * ROWS


def dot(a, b, contract=((1,), (0,))):
    return lax.dot_general(a, b, (contract, ((), ())), preferred_element_type=jnp.float32)


def three_parts(value):
    high = value.astype(jnp.bfloat16)
    rest = value - high.astype(jnp.float32)
    middle = rest.astype(jnp.bfloat16)
    low = (rest - middle.astype(jnp.float32)).astype(jnp.bfloat16)
    return high, middle, low


def attend_kernel(n_queries, n_chunks, counted, *refs):
    q_refs, chunks = refs[:n_queries], refs[n_queries : n_queries + n_chunks]
    out_ref = refs[n_queries + n_chunks]
    query, query_rope, scores, weights = refs[-4:]
    rows = LATENT
    lane = lax.broadcasted_iota(jnp.int32, (BLOCK, LANES), 1)
    query_rope[...] = jnp.where(lane == ROPE, 1.0, 0.0).astype(jnp.bfloat16)
    own_lane = lax.broadcasted_iota(jnp.int32, (ROWS, LANES), 1)
    own_row = lax.broadcasted_iota(jnp.int32, (ROWS, LANES), 0)
    if counted:
        count = jnp.zeros((EXTRA, LANES), jnp.float32)
        for c in range(n_chunks):
            count = count + chunks[c][rows + ROPE :, :LANES].astype(jnp.float32)
        refs[n_queries + n_chunks + 1][...] = count
    owners = [q_ref.at[i] for q_ref in q_refs for i in range(q_ref.shape[0])]
    for i in range(OWNERS):
        for j in range(4):
            query[i * ROWS : (i + 1) * ROWS, j * LANES : (j + 1) * LANES] = owners[i][
                j * ROWS : (j + 1) * ROWS, :
            ]
        both = owners[i][4 * ROWS :, :]
        query_rope[i * ROWS : i * ROWS + 16, :ROPE] = both[:, :ROPE]
        query_rope[i * ROWS + 16 : (i + 1) * ROWS, :ROPE] = both[:, ROPE:]
    half = n_chunks // 2

    def score(c):
        s = dot(query[...], chunks[c][:rows, :], ((1,), (1,)))
        s = s + dot(query_rope[:, : ROPE + EXTRA], chunks[c][rows:, :])
        scores[:, c * rows : (c + 1) * rows] = s
        tiles = [s[:, j * LANES : (j + 1) * LANES] for j in range(rows // LANES)]
        return functools.reduce(jnp.maximum, tiles)

    def weigh(c, peak):
        p = jnp.exp2((scores[:, c * rows : (c + 1) * rows] - peak) * SCALE2)
        weights[:, c * rows : (c + 1) * rows] = p.astype(jnp.bfloat16)
        tiles = [p[:, j * LANES : (j + 1) * LANES] for j in range(rows // LANES)]
        return sum(tiles[1:], tiles[0])

    def value(c):
        return dot(weights[:, c * rows : (c + 1) * rows], chunks[c][:rows, :])

    peak_a = functools.reduce(jnp.maximum, [score(c) for c in range(half)])
    peak_a = jnp.max(peak_a, axis=1, keepdims=True)
    peak_b, total_a = None, None
    for c in range(half):
        part = score(half + c)
        peak_b = part if peak_b is None else jnp.maximum(peak_b, part)
        part = weigh(c, peak_a)
        total_a = part if total_a is None else total_a + part
    peak_b = jnp.max(peak_b, axis=1, keepdims=True)
    latent_a, total_b = None, None
    for c in range(half):
        part = value(c)
        latent_a = part if latent_a is None else latent_a + part
        part = weigh(half + c, peak_b)
        total_b = part if total_b is None else total_b + part
    latent_b = sum((value(c) for c in range(half + 1, n_chunks)), value(half))
    peak = jnp.maximum(peak_a, peak_b)
    keep_a = jnp.exp2((peak_a - peak) * SCALE2)
    keep_b = jnp.exp2((peak_b - peak) * SCALE2)
    total_a = jnp.sum(total_a, axis=1, keepdims=True) * keep_a
    total_b = jnp.sum(total_b, axis=1, keepdims=True) * keep_b
    total = total_a + total_b
    latent = latent_a * (keep_a / total) + latent_b * (keep_b / total)
    latent = latent.astype(jnp.bfloat16)
    lse = peak * SCALE2 + jnp.log2(total)
    for i in range(OWNERS):
        mine = slice(i * ROWS, (i + 1) * ROWS)
        for j in range(4):
            out_ref[i, j * ROWS : (j + 1) * ROWS, :] = latent[mine, j * LANES : (j + 1) * LANES]
        line = jnp.where(own_lane == own_row, lse[mine, :], 0.0)
        out_ref[i, 4 * ROWS :, :] = lines_of(jnp.sum(line, axis=0, keepdims=True))


def lines_of(line):
    parts = [p.astype(jnp.float32) for p in three_parts(line)]
    pad = jnp.zeros((EXTRA - 3, LANES), jnp.float32)
    return jnp.concatenate(parts + [pad], axis=0).astype(jnp.bfloat16)


def attend(queries, chunks, counted=False):
    vmem = pl.BlockSpec(memory_space=pltpu.VMEM)
    n = len(chunks)
    return pl.pallas_call(
        functools.partial(attend_kernel, len(queries), n, counted),
        out_shape=[
            jax.ShapeDtypeStruct((OWNERS, O_ROWS, LANES), jnp.bfloat16),
            jax.ShapeDtypeStruct((EXTRA, LANES), jnp.float32),
        ][: 2 if counted else 1],
        in_specs=[vmem] * (len(queries) + n),
        out_specs=[vmem] * (2 if counted else 1),
        scratch_shapes=[
            pltpu.VMEM((BLOCK, LATENT), jnp.bfloat16),
            pltpu.VMEM((BLOCK, LANES), jnp.bfloat16),
            pltpu.VMEM((BLOCK, n * LATENT), jnp.float32),
            pltpu.VMEM((BLOCK, n * LATENT), jnp.bfloat16),
        ],
        compiler_params=pltpu.CompilerParams(vmem_limit_bytes=14 * 2**20),
        cost_estimate=pl.CostEstimate(
            flops=BLOCK * n * LATENT * 2 * 1280, bytes_accessed=2**20, transcendentals=0
        ),
        name="attend",
    )(*queries, *chunks)


def merge_kernel(n_pieces, *refs):
    pieces, outs = refs[:n_pieces], refs[n_pieces:]
    place = lax.axis_index("z")
    n = pieces[0].shape[0]
    own_lane = lax.broadcasted_iota(jnp.int32, (ROWS, LANES), 1)
    diagonal = own_lane == lax.broadcasted_iota(jnp.int32, (ROWS, LANES), 0)
    owners = [lax.rem(place - 2 * (i // 2) + n, n) for i in range(n)]
    owners = [z + (i % 2) * (1 - 2 * lax.rem(z, 2)) for i, z in enumerate(owners)]
    blocks = [outs[0].at[z] for z in owners]
    for i, out in enumerate(blocks):
        lses = []
        for piece in pieces:
            parts = piece[i, 4 * ROWS :, :].astype(jnp.float32)
            lses.append(parts[0:1, :] + parts[1:2, :] + parts[2:3, :])
        peak = functools.reduce(jnp.maximum, lses)
        shares = [jnp.exp2(lse - peak) for lse in lses]
        total = sum(shares[1:], shares[0])
        out[4 * ROWS :, :] = lines_of(peak + jnp.log2(total))
        shares = [
            jnp.sum(jnp.where(diagonal, share / total, 0.0), axis=1, keepdims=True)
            for share in shares
        ]
        for j in range(4):
            mine = slice(j * ROWS, (j + 1) * ROWS)
            latent = sum(p[i, mine, :].astype(jnp.float32) * s for p, s in zip(pieces, shares))
            out[mine, :] = latent.astype(jnp.bfloat16)


def merge(pieces, groups):
    vmem = pl.BlockSpec(memory_space=pltpu.VMEM)
    n, rest = pieces[0].shape[0], pieces[0].shape[1:]
    return pl.pallas_call(
        functools.partial(merge_kernel, len(pieces)),
        out_shape=[jax.ShapeDtypeStruct((n // groups, *rest), jnp.bfloat16)] * groups,
        in_specs=[vmem] * len(pieces),
        out_specs=[vmem] * groups,
        compiler_params=pltpu.CompilerParams(vmem_limit_bytes=8 * 2**20),
        name="merge",
    )(*pieces)


def pack_query_kernel(lat_ref, rope_ref, out_ref, packed):
    tokens, heads = lat_ref.shape[:2]
    for t in range(tokens):
        lat = lat_ref[t].astype(jnp.float32)
        for j in range(4):
            first = j * ROWS + t * heads
            packed[first : first + heads, :] = lat[:, j * LANES : (j + 1) * LANES]
        first = 4 * ROWS + (t % (tokens // 2)) * heads
        side = (t // (tokens // 2)) * ROPE
        packed[first : first + heads, side : side + ROPE] = rope_ref[t].astype(jnp.float32)
    block = packed[...].astype(jnp.bfloat16)
    for i in range(out_ref.shape[0]):
        out_ref[i] = block


def pack_query(q_latent, q_rope, copies):
    vmem = pl.BlockSpec(memory_space=pltpu.VMEM)
    return pl.pallas_call(
        pack_query_kernel,
        out_shape=jax.ShapeDtypeStruct((copies, Q_ROWS, LANES), jnp.bfloat16),
        in_specs=[vmem] * 2,
        out_specs=vmem,
        scratch_shapes=[pltpu.VMEM((Q_ROWS, LANES), jnp.float32)],
        compiler_params=pltpu.CompilerParams(vmem_limit_bytes=8 * 2**20),
        name="pack_query",
    )(q_latent, q_rope)


def pack_cache_kernel(valid, accepted, lat, rope, out, packed, valid_ref, accepted_ref, sems):
    parts = 4
    step = LATENT // parts
    spans = [slice(i * step, (i + 1) * step) for i in range(parts)]
    loads = [
        pltpu.make_async_copy(lat.at[span], packed.at[span], sems.at[i])
        for i, span in enumerate(spans)
    ]
    last = slice(LATENT, LATENT + ROPE + EXTRA)
    rest = [
        pltpu.make_async_copy(rope, packed.at[LATENT : LATENT + ROPE], sems.at[parts]),
        pltpu.make_async_copy(valid, valid_ref, sems.at[parts + 1]),
        pltpu.make_async_copy(accepted, accepted_ref, sems.at[parts + 2]),
    ]
    stores = [
        pltpu.make_async_copy(packed.at[span], out.at[span], sems.at[parts + 3 + i])
        for i, span in enumerate(spans + [last])
    ]
    for copy in rest + loads:
        copy.start()
    for copy in rest:
        copy.wait()
    limit = valid_ref[0] - lax.axis_index(SEQ + BLK) * LATENT
    count = sum(accepted_ref[i] for i in range(accepted_ref.shape[0]))
    lane = lax.broadcasted_iota(jnp.int32, (EXTRA, LATENT), 1)
    row = lax.broadcasted_iota(jnp.int32, (EXTRA, LATENT), 0)
    dead = jnp.where((row == 0) & (lane >= limit), NEG, 0.0)
    extra = jnp.where(row == 1, count.astype(jnp.float32), dead)
    packed[LATENT + ROPE :, :] = extra.astype(jnp.bfloat16)
    for load, store in zip(loads, stores):
        load.wait()
        store.start()
    stores[-1].start()
    for store in stores:
        store.wait()


def pack_cache(valid_length, accepted, cache_latent, cache_rope):
    hbm = pl.BlockSpec(memory_space=pltpu.HBM)
    rows = LATENT + ROPE + EXTRA
    return pl.pallas_call(
        pack_cache_kernel,
        out_shape=jax.ShapeDtypeStruct((rows, LATENT), jnp.bfloat16),
        in_specs=[hbm] * 4,
        out_specs=hbm,
        scratch_shapes=[
            pltpu.VMEM((rows, LATENT), jnp.bfloat16),
            pltpu.SMEM((1,), jnp.int32),
            pltpu.SMEM(accepted.shape, jnp.int32),
            pltpu.SemaphoreType.DMA((12,)),
        ],
        compiler_params=pltpu.CompilerParams(vmem_limit_bytes=60 * 1024 * 2**10 - 660 * 2**10),
        name="pack_cache",
    )(valid_length.reshape(1), accepted, cache_latent, cache_rope)


def draft_kernel(q_ref, d_lat_ref, d_rope_ref, tree_ref, latent_ref, peak_ref, total_ref):
    q_ref = q_ref.at[0]
    query = jnp.concatenate([q_ref[j * ROWS : (j + 1) * ROWS, :] for j in range(4)], axis=1)
    both = q_ref[4 * ROWS :, :]
    query_rope = jnp.concatenate([both[:, :ROPE], both[:, ROPE:]], axis=0)
    draft = d_lat_ref[...]
    score = dot(query, draft, ((1,), (1,))) + dot(query_rope, d_rope_ref[...])
    score = jnp.where(tree_ref[...] == 1, score * SCALE2, NEG)
    peak = jnp.max(score, axis=1, keepdims=True)
    weight = jnp.exp2(score - peak)
    latent_ref[...] = dot(weight.astype(jnp.bfloat16), draft)
    peak_ref[...] = jnp.broadcast_to(peak, (ROWS, LANES))
    total_ref[...] = jnp.broadcast_to(jnp.sum(weight, axis=1, keepdims=True), (ROWS, LANES))


def attend_draft(own, draft_latent, draft_rope, tree):
    vmem = pl.BlockSpec(memory_space=pltpu.VMEM)
    return pl.pallas_call(
        draft_kernel,
        out_shape=[
            jax.ShapeDtypeStruct((ROWS, LATENT), jnp.float32),
            jax.ShapeDtypeStruct((ROWS, LANES), jnp.float32),
            jax.ShapeDtypeStruct((ROWS, LANES), jnp.float32),
        ],
        in_specs=[vmem] * 4,
        out_specs=[vmem] * 3,
        compiler_params=pltpu.CompilerParams(vmem_limit_bytes=8 * 2**20),
        cost_estimate=pl.CostEstimate(flops=10**9, bytes_accessed=2**20, transcendentals=0),
        name="draft",
    )(own, draft_latent, draft_rope, tree)


def finish_kernel(tokens, heads, pieces_ref, d_lat_ref, d_peak_ref, d_total_ref, w_ref, out_ref):
    n = pieces_ref.shape[0]
    lses = []
    for i in range(n):
        parts = pieces_ref[i, 4 * ROWS :, :].astype(jnp.float32)
        lses.append(parts[0:1, :] + parts[1:2, :] + parts[2:3, :])
    own_lane = lax.broadcasted_iota(jnp.int32, (ROWS, LANES), 1)
    diagonal = own_lane == lax.broadcasted_iota(jnp.int32, (ROWS, LANES), 0)
    draft_peak = d_peak_ref[:, :1]
    lses = [jnp.sum(jnp.where(diagonal, lse, 0.0), axis=1, keepdims=True) for lse in lses]
    peak = functools.reduce(jnp.maximum, lses, draft_peak)
    keep = jnp.exp2(draft_peak - peak)
    shares = [jnp.exp2(lse - peak) for lse in lses]
    total = d_total_ref[:, :1] * keep + sum(shares[1:], shares[0])
    latent = d_lat_ref[...] * keep
    for i in range(n):
        piece = [pieces_ref[i, j * ROWS : (j + 1) * ROWS, :] for j in range(4)]
        latent = latent + shares[i] * jnp.concatenate(piece, axis=1).astype(jnp.float32)
    latent = latent / total
    high = latent.astype(jnp.bfloat16)
    low = (latent - high.astype(jnp.float32)).astype(jnp.bfloat16)
    head = lax.broadcasted_iota(jnp.int32, (ROWS, VDIM), 0) % heads
    value = jnp.zeros((ROWS, VDIM), jnp.float32)
    for h in range(heads):
        value = jnp.where(head == h, dot(high, w_ref[h]) + dot(low, w_ref[h]), value)
    for t in range(tokens):
        out_ref[t] = value[t * heads : (t + 1) * heads, :].astype(out_ref.dtype)


def finish(pieces, draft, w_value, tokens, heads):
    vmem = pl.BlockSpec(memory_space=pltpu.VMEM)
    return pl.pallas_call(
        functools.partial(finish_kernel, tokens, heads),
        out_shape=jax.ShapeDtypeStruct((tokens, heads, VDIM), jnp.bfloat16),
        in_specs=[vmem] * 5,
        out_specs=vmem,
        compiler_params=pltpu.CompilerParams(vmem_limit_bytes=8 * 2**20),
        name="finish",
    )(pieces, *draft, w_value)


def both_ways(n, step):
    return [
        (i * 2 + core, (i + (step if core == 0 else -step)) % n * 2 + core)
        for i in range(n)
        for core in range(2)
    ]


def shift(value, axis, step):
    return lax.ppermute(value, (axis, "core"), both_ways(lax.axis_size(axis), step))


def across(value, axis):
    n = lax.axis_size(axis)
    return lax.ppermute(value, axis, [(i, (i + n // 2) % n) for i in range(n)])


def pair(value, axis):
    return lax.ppermute(value, axis, [(i, i ^ 1) for i in range(lax.axis_size(axis))])


def rotate(value, axis, step):
    n = lax.axis_size(axis)
    return lax.ppermute(value, axis, [(i, (i + step) % n) for i in range(n)])


def other_core(value):
    return lax.ppermute(value, "core", [(0, 1), (1, 0)])


def shards(
    q_latent,
    q_rope,
    cache_latent,
    cache_rope,
    draft_latent,
    draft_rope,
    ancestors,
    valid_length,
    accepted,
    w_value,
):
    tokens, heads = q_latent.shape[:2]
    nz = lax.axis_size("z")

    packed = pack_query(q_latent, q_rope.transpose(0, 2, 1), 1)
    own = pack_cache(valid_length, accepted, cache_latent, cache_rope)
    ahead = shift(own, "x", 1)
    behind = shift(own, "x", -1)
    far = shift(ahead, "x", 1)
    near = jnp.concatenate([packed, pair(packed, "z")], axis=0)
    turned = [near]
    for step in range(2, nz, 2):
        turned.append(rotate(near, "z", step))
    near = jnp.concatenate(turned, axis=0)
    q_far = across(near, "y")
    q_ahead = shift(near, "y", 1)
    q_behind = shift(near, "y", -1)
    mine = (own, ahead, behind, far)
    chunks = list(mine)
    for chunk in mine:
        chunks.append(other_core(chunk))

    part_far, counts = attend((q_far,), chunks, counted=True)
    (part_ahead,) = attend((q_ahead,), chunks)
    (part_behind,) = attend((q_behind,), chunks)
    (part_near,) = attend((near,), chunks)
    from_far = across(part_far, "y")
    from_ahead = shift(part_ahead, "y", -1)
    from_behind = shift(part_behind, "y", 1)
    (pieces,) = merge((part_near, from_far, from_ahead, from_behind), 1)
    pieces = lax.all_to_all(pieces, "z", 0, 0, tiled=True)
    tree = lax.dynamic_slice_in_dim(ancestors, lax.axis_index(BLK) * tokens, tokens, 0)
    tree = jnp.repeat(tree, heads, axis=0)
    draft = attend_draft(packed, draft_latent, draft_rope, tree)
    attended = finish(pieces, draft, w_value, tokens, heads)
    return (attended, counts[1, 0].astype(jnp.int32))


def solution(mesh):
    finer = Mesh(mesh.devices.reshape(8, 4, 4, 2), SEQ + BLK)

    return jax.shard_map(
        shards,
        mesh=finer,
        in_specs=(
            P(BLK, SEQ, None),
            P(BLK, None, SEQ),
            P(SEQ + BLK, None),
            P(None, SEQ + BLK),
            P(),
            P(),
            P(),
            P(),
            P(BLK),
            P(SEQ, None, None),
        ),
        out_specs=(P(BLK, SEQ, None), P()),
        check_vma=False,
    )
```
